32 devices in a mesh: pitch: 4 (over z), inst: 4 (over y, core), span: 2 (over x).
Axes of the slice: x: 2, y: 2, z: 4, core: 2. Of those that a mesh axis runs over, the one named last changes fastest.
Arguments:
- donor_state: float32 [2, 20, 5, 128, 512], P(None, 'inst', None, 'span', 'pitch'), may hold values from -6 to 6
- time_shift: float32 [2, 17, 17], replicated, may hold values from -1.5 to 1.5
- face_shift: int32 [17], replicated, may hold values from 0 to 255, as said below
- weights: float32 [2, 4, 512], P(None, None, 'pitch'), may hold values from 0.1 to 0.5
- offsets: int32 [2, 4], replicated, may hold values from -3 to 3
Outputs:
- received: float32 [2, 20, 5, 128, 512], P(None, 'inst', None, 'span', 'pitch')
The draws below stay inside these ranges and needn't reach their ends.
Inputs may be any that keep to these rules, and one draw needn't show every extreme that they name: `face_shift`: at least one instance has a shift of 192 or more.
All inputs are finite; a program needn't handle non-finite values.
Results may differ from the reference program's by a relative error of at most 0.00007.
Values sent between devices are 32-bit elements; how exact they have to be, the bound alone decides.
A program may use at most 128 MiB of HBM per device.

```python
import math
import jax
import jax.numpy as jnp
from jax import lax

INSTANCES = 17
VARS = 5
BAND = 4
HALO = 3
PITCH_DEV = 128
REACH = 2
INST_PAD = 20
PITCH = 512
SPAN = 128


def draw_face_shift(key, part):
    limit = REACH * PITCH_DEV
    base = jax.random.randint(jax.random.fold_in(key, 11), (INSTANCES,), 0, limit, dtype=jnp.int32)
    chosen = jax.random.randint(jax.random.fold_in(key, 12), (), 0, INSTANCES, dtype=jnp.int32)
    high = limit - 1 - jax.random.randint(jax.random.fold_in(key, 13), (), 0, PITCH_DEV // 2, dtype=jnp.int32)
    places = jnp.arange(INSTANCES, dtype=jnp.int32)
    return jnp.where(places == chosen, high, base).astype(jnp.int32)


def place_ends(entries, stream_key, smallest, high):
    place = [jax.random.randint(jax.random.fold_in(stream_key, axis), (), 0, length) for axis, length in enumerate(entries.shape)]
    widest = entries.shape.index(max(entries.shape))
    next_to = place[:widest] + [(place[widest] + 1) % entries.shape[widest]] + place[widest + 1:]
    return entries.at[tuple(place)].set(smallest).at[tuple(next_to)].set(high)


def block_scale(key, dims, shards, low, high):
    def one(position, blocks):
        draws = jax.random.uniform(jax.random.fold_in(jax.random.fold_in(key, 6), position), (blocks,), jnp.float32, low / len(shards), high / len(shards))
        return jnp.repeat(jnp.exp(draws), dims[position] // blocks).reshape((-1,) + (1,) * (len(dims) - position - 1))

    gain = one(*shards[0])
    for cut in shards[1:]:
        gain = gain * one(*cut)
    return gain


def centred(own_key, extent, deviation, reach, cuts=(), held_as=jnp.bfloat16):
    gain = block_scale(own_key, extent, cuts, -0.22, 0.18) if cuts else 1.0
    values = jax.random.normal(own_key, extent, jnp.float32) * deviation * gain
    return jnp.minimum(jnp.maximum(values, -reach), reach).astype(held_as)


def setup_inputs(seed: int = 0) -> dict:
    seeds = jax.random.split(jax.random.key(seed), 6)
    donor_state = centred(seeds[0], (2, INST_PAD, VARS, SPAN, PITCH), 1.0, 6.0, ((1, 4), (3, 2), (4, 4)), jnp.float32)
    time_shift = centred(seeds[1], (2, INSTANCES, INSTANCES), 0.25, 1.5, (), jnp.float32)
    face_shift = draw_face_shift(jax.random.fold_in(seeds[5], 71), 0)
    weights = jnp.clip(jnp.exp(math.log(0.5) - 1.609438 * jax.random.uniform(seeds[3], (2, BAND, PITCH), jnp.float32) ** block_scale(seeds[3], (2, BAND, PITCH), ((2, 4),), -0.2, 0.2)), 0.1, 0.5)
    offsets = place_ends(jax.random.randint(seeds[4], (2, BAND), 0 - HALO, HALO + 1), jax.random.fold_in(seeds[4], 1), 0 - HALO, HALO).astype(jnp.int32)
    return {"donor_state": donor_state, "time_shift": time_shift, "face_shift": face_shift, "weights": weights, "offsets": offsets}


def roll_one(field, amount):
    return jnp.roll(field, -amount, axis=-1)


def reference(donor_state, time_shift, face_shift, weights, offsets):
    donor = donor_state[:, :INSTANCES][::-1]
    resampled = jnp.einsum("rmk,rkvsp->rmvsp", time_shift, donor, precision=lax.Precision.HIGHEST)
    result = []
    for row in range(2):
        sign = 1 - 2 * row
        summed = jnp.zeros(resampled.shape[1:], jnp.float32)
        for member in range(BAND):
            amounts = (sign * face_shift + offsets[row, member]).astype(jnp.int32)
            moved = jax.vmap(roll_one)(resampled[row], amounts)
            summed = summed + weights[row, member][None, None, None, :] * moved
        result.append(summed)
    stacked = jnp.stack(result)
    filler = jnp.zeros((2, INST_PAD - INSTANCES) + stacked.shape[2:], jnp.float32)
    return jnp.concatenate([stacked, filler], axis=1)
```

```python
import jax
import jax.numpy as jnp
from jax import lax
from jax.experimental import pallas as pl
from jax.experimental.pallas import tpu as pltpu
from jax.sharding import PartitionSpec as P

MESH = pl.DeviceIdType.MESH
TILE = 8
EDGE = 4
REACH = 3
LEAD = 8
BUDGETS = (
    (9, 4), (9, 5), (11, 4), (10, 5), (9, 6), (10, 6), (12, 5), (9, 7), (9, 8), (13, 7), (10, 10),
)


def lanes_rolled(value, amount):
    return pltpu.roll(value, amount, 1)


def make_general(insts, strips, count, inst_dev, variables, span_dev, width, band_members):
    band = span_dev // insts
    parts = band // TILE
    chunks = variables * parts
    rounds = max(0, (strips // 2 - 1).bit_length())
    whole_owners, rest = divmod(count, inst_dev)
    slots = insts * inst_dev
    far = sorted({step % strips for bit in range(rounds) for step in (2**bit, -(2**bit))}
                 | {step % strips for step in (1, -1, 2, -2)} - {0})

    def kernel(time_hbm, shift_hbm, offset_hbm, weight_hbm, donor_ref, out_ref,
               time_ref, shift_ref, offset_ref, weight_ref, small_sem, raw, states, edges_out, edges_in, finished,
               in_send, in_recv, local_sem, move_send, move_recv, edge_send, edge_recv,
               out_send, out_recv, keep_sem):
        inst = lax.axis_index("inst")
        strip = lax.axis_index("pitch")

        def peer(step):
            return lax.rem(inst + step, insts)

        def along(step):
            return lax.rem(strip + (step % strips), strips)

        def place(chunk):
            variable = chunk // parts
            return variable, (chunk - variable * parts) * TILE

        def rows_of(owner, inner):
            return pl.ds(pl.multiple_of(owner * band + inner, TILE), TILE)

        def bring(chunk, step, size):
            variable, inner = place(chunk)
            target = peer(step)
            return pltpu.make_async_remote_copy(
                src_ref=donor_ref.at[:, pl.ds(0, size), variable, rows_of(target, inner), :],
                dst_ref=raw.at[chunk, :, pl.ds(inst * inst_dev, size)],
                send_sem=in_send.at[chunk, step - 1],
                recv_sem=in_recv.at[chunk, step - 1],
                device_id={"inst": target},
                device_id_type=MESH,
            )

        def bring_own(chunk):
            variable, inner = place(chunk)
            return pltpu.make_async_copy(
                donor_ref.at[:, :, variable, rows_of(inst, inner), :],
                raw.at[chunk, :, pl.ds(inst * inst_dev, inst_dev)],
                local_sem.at[chunk],
            )

        def move(chunk, row, turn):
            step = 2**turn if turn < rounds else 1
            return pltpu.make_async_remote_copy(
                src_ref=states.at[2 * turn, chunk, row],
                dst_ref=states.at[2 * turn + 1, chunk, row],
                send_sem=move_send.at[chunk, row, turn],
                recv_sem=move_recv.at[chunk, row, turn],
                device_id={"pitch": along(-step if row == 0 else step)},
                device_id_type=MESH,
            )

        def edge_step(row, side):
            if row == 0:
                return -2 if side == 0 else 1
            return -1 if side == 0 else 2

        def move_edge(chunk, row, side):
            return pltpu.make_async_remote_copy(
                src_ref=edges_out.at[chunk, row, side],
                dst_ref=edges_in.at[chunk, row, side],
                send_sem=edge_send.at[chunk, row, side],
                recv_sem=edge_recv.at[chunk, row, side],
                device_id={"pitch": along(edge_step(row, side))},
                device_id_type=MESH,
            )

        def give(chunk, step, size):
            variable, inner = place(chunk)
            target = peer(step)
            return pltpu.make_async_remote_copy(
                src_ref=finished.at[chunk, :, pl.ds(target * inst_dev, size)],
                dst_ref=out_ref.at[:, pl.ds(0, size), variable, rows_of(inst, inner), :],
                send_sem=out_send.at[chunk, step - 1],
                recv_sem=out_recv.at[chunk, step - 1],
                device_id={"inst": target},
                device_id_type=MESH,
            )

        def keep(chunk, size):
            variable, inner = place(chunk)
            return pltpu.make_async_copy(
                finished.at[chunk, :, pl.ds(inst * inst_dev, size)],
                out_ref.at[:, pl.ds(0, size), variable, rows_of(inst, inner), :],
                keep_sem.at[chunk],
            )

        def by_owner(owner, act):
            @pl.when(owner < whole_owners)
            def _():
                act(inst_dev)

            if rest:
                @pl.when(owner == whole_owners)
                def _():
                    act(rest)

        def select_bit(row, index, bit):
            if bit < 0:
                return None
            level = jnp.full((TILE, width), shift_ref[index] // width, jnp.int32)
            return (level & (1 << bit)) != 0

        def resample(chunk):
            for row in range(2):
                donors = [raw[chunk, 1 - row, k] for k in range(count)]

                for m in range(count):
                    total = time_ref[m, row, 0] * donors[0]
                    for k in range(1, count):
                        total = total + time_ref[m, row, k] * donors[k]
                    states[0, chunk, row, m] = total

        def send_turn(chunk, turn):
            for row in range(2):
                move(chunk, row, turn).start()

        def pack_edges(chunk):
            lane = lax.broadcasted_iota(jnp.int32, (TILE, width), 1)
            for row in range(2):
                low = jnp.zeros((TILE, width), jnp.float32)
                high = jnp.zeros((TILE, width), jnp.float32)
                for m in range(count):
                    value = states[2 * rounds, chunk, row, m]
                    here = (lane >= EDGE * m) & (lane < EDGE * (m + 1))
                    low = jnp.where(here, lanes_rolled(value, EDGE * m), low)
                    high = jnp.where(here, lanes_rolled(value, (EDGE * (m + 1)) % width), high)
                edges_out[chunk, row, 0] = low
                edges_out[chunk, row, 1] = high

        def take_turn(chunk, turn):
            for row in range(2):
                move(chunk, row, turn).wait_recv()
                for m in range(count):
                    states[2 * turn + 2, chunk, row, m] = jnp.where(
                        select_bit(row, m, turn),
                        states[2 * turn + 1, chunk, row, m],
                        states[2 * turn, chunk, row, m],
                    )

        def send_fine(chunk):
            send_turn(chunk, rounds)
            pack_edges(chunk)
            for row in range(2):
                for side in range(2):
                    move_edge(chunk, row, side).start()

        def interpolate(chunk):
            lane = lax.broadcasted_iota(jnp.int32, (TILE, width), 1)
            for row in range(2):
                move(chunk, row, rounds).wait_recv()
                for side in range(2):
                    move_edge(chunk, row, side).wait_recv()
                above = edges_in[chunk, row, 0]
                below = edges_in[chunk, row, 1]
                weight = [jnp.broadcast_to(weight_ref[row, b][None, :], (TILE, width)) for b in range(band_members)]
                for m in range(count):
                    own = states[2 * rounds, chunk, row, m]
                    near = states[2 * rounds + 1, chunk, row, m]
                    first, second = (own, near) if row == 0 else (near, own)
                    after = lanes_rolled(above, (width - EDGE * m) % width)
                    before = lanes_rolled(below, (2 * width - EDGE * (m + 1)) % width)
                    inner = lax.rem(shift_ref[m], width)
                    base = inner if row == 0 else width - inner
                    total = None
                    for b in range(band_members):
                        start = base + offset_ref[row, b]
                        at = jnp.full((TILE, width), start, jnp.int32)
                        ahead = jnp.where(at < 0, first, jnp.where(at < width, second, after))
                        behind = jnp.where(at < 0, before, jnp.where(at < width, first, second))
                        turn = at & (width - 1)
                        mixed = jnp.where(lane >= turn, behind, ahead)
                        back = lax.rem(2 * width - start, width)
                        part = weight[b] * lanes_rolled(mixed, back)
                        total = part if total is None else total + part
                    finished[chunk, row, m] = total

        small = [
            pltpu.make_async_copy(source, target, small_sem.at[n])
            for n, (source, target) in enumerate(((shift_hbm, shift_ref), (offset_hbm, offset_ref),
                                                  (time_hbm, time_ref), (weight_hbm, weight_ref)))
        ]
        for copy in small:
            copy.start()

        barrier = pltpu.get_barrier_semaphore()
        for step in range(1, insts):
            pl.semaphore_signal(barrier, inc=1, device_id={"inst": peer(step)}, device_id_type=MESH)
        for step in far:
            pl.semaphore_signal(barrier, inc=1, device_id={"pitch": along(step)}, device_id_type=MESH)
        pl.semaphore_wait(barrier, insts - 1 + len(far))

        @pl.loop(0, chunks)
        def _(chunk):
            bring_own(chunk).start()
            for step in range(1, insts):
                by_owner(inst, lambda size, step=step: bring(chunk, step, size).start())

        for copy in small:
            copy.wait()
        lead = rounds + 1

        @pl.loop(0, chunks + lead)
        def _(tick):
            @pl.when(tick < chunks)
            def _():
                bring_own(tick).wait()
                for step in range(1, insts):
                    by_owner(peer(insts - step), lambda size, step=step: bring(tick, step, size).wait_recv())
                resample(tick)
                if rounds:
                    send_turn(tick, 0)
                else:
                    send_fine(tick)

            for turn in range(rounds):
                @pl.when((tick >= turn + 1) & (tick < chunks + turn + 1))
                def _(turn=turn):
                    chunk = tick - turn - 1
                    take_turn(chunk, turn)
                    if turn + 1 < rounds:
                        send_turn(chunk, turn + 1)
                    else:
                        send_fine(chunk)

            @pl.when(tick >= lead)
            def _():
                chunk = tick - lead
                interpolate(chunk)
                for step in range(1, insts):
                    by_owner(peer(step), lambda size, step=step: give(chunk, step, size).start())
                by_owner(inst, lambda size: keep(chunk, size).start())

        @pl.loop(0, chunks)
        def _(chunk):
            for step in range(1, insts):
                by_owner(inst, lambda size, step=step: bring(chunk, step, size).wait_send())
                by_owner(peer(step), lambda size, step=step: give(chunk, step, size).wait_send())
                by_owner(inst, lambda size, step=step: give(chunk, step, size).wait_recv())
            by_owner(inst, lambda size: keep(chunk, size).wait())
            for row in range(2):
                for turn in range(rounds + 1):
                    move(chunk, row, turn).wait_send()
                for side in range(2):
                    move_edge(chunk, row, side).wait_send()

    vmem, dma = pltpu.VMEM, pltpu.SemaphoreType.DMA
    legs = rounds + 1
    scratch = [
        pltpu.SMEM((count, 2, count), jnp.float32),
        pltpu.SMEM((count,), jnp.int32),
        pltpu.SMEM((2, band_members), jnp.int32),
        vmem((2, band_members, width), jnp.float32),
        dma((4,)),
        vmem((chunks, 2, slots, TILE, width), jnp.float32),
        vmem((2 * rounds + 2, chunks, 2, count, TILE, width), jnp.float32),
        vmem((chunks, 2, 2, TILE, width), jnp.float32),
        vmem((chunks, 2, 2, TILE, width), jnp.float32),
        vmem((chunks, 2, slots, TILE, width), jnp.float32),
        dma((chunks, insts - 1)), dma((chunks, insts - 1)), dma((chunks,)),
        dma((chunks, 2, legs)), dma((chunks, 2, legs)),
        dma((chunks, 2, 2)), dma((chunks, 2, 2)),
        dma((chunks, insts - 1)), dma((chunks, insts - 1)), dma((chunks,)),
    ]
    return kernel, scratch


def make_compact(insts, strips, count, inst_dev, variables, span_dev, width, members, near, far):
    band = span_dev // insts
    parts = band // TILE
    shift_bits = width.bit_length() - 1
    items = 2 * variables * parts
    whole_owners, rest = divmod(count, inst_dev)
    slots = insts * inst_dev
    tiles = near + far
    first_tile, piece_tiles = (0, near), (near, far)

    def kernel(time_hbm, shift_hbm, offset_hbm, weight_hbm, donor_ref, out_ref,
               time_ref, shift_ref, offset_ref, weight_ref, small_sem, stage, stage_sem, raw, states, finished,
               packed_out, packed_in, edge_out, edge_in, opened, edge_now, tile_ids, edge_ids, table,
               in_send, in_recv, near_send, near_recv, far_send, far_recv, edge_send, edge_recv,
               out_send, out_recv, keep_sem):
        inst = lax.axis_index("inst")
        strip = lax.axis_index("pitch")

        def peer(step):
            return lax.rem(inst + step, insts)

        def along(step):
            return lax.rem(strip + strips + step, strips)

        def place(item):
            chunk = item // 2
            variable = chunk // parts
            return item - 2 * chunk, variable, (chunk - variable * parts) * TILE

        def rows_of(owner, inner):
            return pl.ds(pl.multiple_of(owner * band + inner, TILE), TILE)

        def stage_in(row, variable):
            return pltpu.make_async_copy(
                donor_ref.at[row, :, variable], stage.at[row, :, variable], stage_sem.at[row, variable]
            )

        def bring(item, step, size):
            row, variable, inner = place(item)
            target = peer(step)
            return pltpu.make_async_remote_copy(
                src_ref=stage.at[1 - row, pl.ds(0, size), variable, rows_of(target, inner), :],
                dst_ref=raw.at[item, pl.ds(inst * inst_dev, size)],
                send_sem=in_send.at[item, step - 1],
                recv_sem=in_recv.at[item, step - 1],
                device_id={"inst": target},
                device_id_type=MESH,
            )

        def move_near(item):
            row = item - 2 * (item // 2)
            return pltpu.make_async_remote_copy(
                src_ref=packed_out.at[item, pl.ds(0, near)],
                dst_ref=packed_in.at[item, pl.ds(0, near)],
                send_sem=near_send.at[item],
                recv_sem=near_recv.at[item],
                device_id={"pitch": along(2 * row - 1)},
                device_id_type=MESH,
            )

        def move_far(item):
            return pltpu.make_async_remote_copy(
                src_ref=packed_out.at[item, pl.ds(near, far)],
                dst_ref=packed_in.at[item, pl.ds(near, far)],
                send_sem=far_send.at[item],
                recv_sem=far_recv.at[item],
                device_id={"pitch": along(2)},
                device_id_type=MESH,
            )

        def move_edge():
            return pltpu.make_async_remote_copy(
                src_ref=edge_out,
                dst_ref=edge_in,
                send_sem=edge_send.at[0],
                recv_sem=edge_recv.at[0],
                device_id={"pitch": along(-1)},
                device_id_type=MESH,
            )

        def give(item, step, size):
            row, variable, inner = place(item)
            target = peer(step)
            return pltpu.make_async_remote_copy(
                src_ref=finished.at[item, pl.ds(target * inst_dev, size)],
                dst_ref=out_ref.at[row, pl.ds(0, size), variable, rows_of(inst, inner), :],
                send_sem=out_send.at[item, step - 1],
                recv_sem=out_recv.at[item, step - 1],
                device_id={"inst": target},
                device_id_type=MESH,
            )

        def keep(item, size):
            row, variable, inner = place(item)
            return pltpu.make_async_copy(
                finished.at[item, pl.ds(inst * inst_dev, size)],
                out_ref.at[row, pl.ds(0, size), variable, rows_of(inst, inner), :],
                keep_sem.at[item],
            )

        def by_owner(owner, act):
            @pl.when(owner < whole_owners)
            def _():
                act(inst_dev)

            if rest:
                @pl.when(owner == whole_owners)
                def _():
                    act(rest)

        def lanes():
            return lax.broadcasted_iota(jnp.int32, (TILE, width), 1)

        def full(value):
            return jnp.full((TILE, width), value, jnp.int32)

        def edge_amount(row, m):
            ends_high = (shift_ref[m] < width) == (row == 0)
            return table[4 * count * 3 + row * count + m] - jnp.where(ends_high, width - EDGE, 0)

        def plan():
            lane = lanes()
            for row in range(2):
                for piece in range(2):
                    begin = jnp.int32(0)
                    for m in range(count):
                        origin = width * (piece + 1)
                        shift = shift_ref[m]
                        low = (shift if row == 0 else 2 * width * (piece + 1) - shift) - REACH - origin
                        start = jnp.clip(low, 0, width)
                        stop = jnp.clip(low + width + 2 * REACH, 0, width)
                        moved = begin - start + width
                        source = (lane - full(moved)) & (width - 1)
                        tile = ((source + full(moved)) >> shift_bits) - 1
                        inside = (source >= full(start)) & (source < full(stop))
                        tile_ids[row, piece, m] = jnp.where(inside, tile, -1)
                        at = ((row * 2 + piece) * count + m) * 3
                        table[at] = moved & (width - 1)
                        tile0 = (moved >> shift_bits) - 1
                        table[at + 1] = jnp.clip(tile0, 0, piece_tiles[piece] - 1) + first_tile[piece]
                        table[at + 2] = jnp.clip(tile0 + 1, 0, piece_tiles[piece] - 1) + first_tile[piece]
                        begin = begin + stop - start
                    if piece == 0:
                        begin = ((begin + (EDGE - 1)) >> 2) << 2
                        owner, spot = jnp.full((TILE, width), -1, jnp.int32), jnp.full((TILE, width), -1, jnp.int32)
                        for m in range(count):
                            shift = shift_ref[m]
                            needed = ((shift < REACH) | (shift + REACH > 2 * width)).astype(jnp.int32)
                            at_lane = begin & (width - 1)
                            here = (lane >= full(at_lane)) & (lane < full(at_lane + EDGE * needed))
                            owner = jnp.where(here, m, owner)
                            spot = jnp.where(here, full(begin >> shift_bits), spot)
                            table[4 * count * 3 + (1 - row) * count + m] = at_lane
                            begin = begin + EDGE * needed
                        edge_ids[1 - row, 0] = owner
                        edge_ids[1 - row, 1] = spot

        def resample(item):
            row = item - 2 * (item // 2)
            donors = [raw[item, k] for k in range(count)]
            for m in range(count):
                total = time_ref[m, row, 0] * donors[0]
                for k in range(1, count):
                    total = total + time_ref[m, row, k] * donors[k]
                states[item, m] = total

        def gather_edges(item, row):
            owner = edge_ids[row, 0]
            edge = jnp.zeros((TILE, width), jnp.float32)
            for m in range(count):
                amount = edge_amount(row, m) & (width - 1)
                edge = jnp.where(owner == m, lanes_rolled(states[item, m], amount), edge)
            return edge

        def pack(item):
            row = item - 2 * (item // 2)
            for piece in (1, 0):
                out = [jnp.zeros((TILE, width), jnp.float32)] * piece_tiles[piece]
                for m in range(count):
                    at = ((row * 2 + piece) * count + m) * 3
                    turned = lanes_rolled(states[item, m], table[at])
                    ids = tile_ids[row, piece, m]
                    out = [jnp.where(ids == t, turned, out[t]) for t in range(piece_tiles[piece])]
                if piece == 0:
                    edge = gather_edges(jnp.maximum(item - 1, 0), 1 - row)
                    spot = edge_ids[1 - row, 1]
                    out = [jnp.where(spot == t, edge, out[t]) for t in range(near)]
                for t in range(piece_tiles[piece]):
                    packed_out[item, first_tile[piece] + t] = out[t]
            wraps = strip == row * (strips - 1)

            @pl.when(wraps)
            def _():
                move_near(item).start()
            move_far(item).start()

            @pl.when(jnp.logical_not(wraps))
            def _():
                move_near(item).start()

        def unpack(row, piece, m, lane):
            at = ((row * 2 + piece) * count + m) * 3
            turn = table[at]
            both = jnp.where(lane >= full(turn), opened[table[at + 1]], opened[table[at + 2]])
            return lanes_rolled(both, (width - turn) & (width - 1))

        def interpolate(item):
            row = item - 2 * (item // 2)
            lane = lanes()

            @pl.when(item == 0)
            def _():
                move_near(item).wait_recv()
            move_far(item).wait_recv()

            @pl.when(item + 1 < items)
            def _():
                move_near(item + 1).wait_recv()
                spot = edge_ids[row, 1]
                edge = jnp.zeros((TILE, width), jnp.float32)
                for t in range(near):
                    edge = jnp.where(spot == t, packed_in[item + 1, t], edge)
                edge_now[...] = edge

            @pl.when(item + 1 == items)
            def _():
                move_edge().wait_recv()
                edge_now[...] = edge_in[...]

            for t in range(tiles):
                opened[t] = packed_in[item, t]
            edge = edge_now[...]
            weight = [jnp.broadcast_to(weight_ref[row, b][None, :], (TILE, width)) for b in range(members)]
            forward = full(row) == 0
            for m in range(count):
                strip0 = states[item, m]
                strip1 = unpack(row, 0, m, lane)
                strip2 = unpack(row, 1, m, lane)
                shift = shift_ref[m]
                strip3 = lanes_rolled(edge, (2 * width - edge_amount(row, m)) & (width - 1))
                large = full(shift) >= width
                line = [jnp.where(large, strip0, strip3), jnp.where(large, strip1, strip0),
                        jnp.where(large, strip2, strip1), jnp.where(large, strip3, strip2)]
                before, first = jnp.where(forward, line[0], line[3]), jnp.where(forward, line[1], line[2])
                second, after = jnp.where(forward, line[2], line[1]), jnp.where(forward, line[3], line[0])
                inner = shift & (width - 1)
                base = jnp.where(row == 0, inner, width - inner)
                total = None
                for b in range(members):
                    start = base + offset_ref[row, b]
                    at = full(start)
                    ahead = jnp.where(at < 0, first, jnp.where(at < width, second, after))
                    behind = jnp.where(at < 0, before, jnp.where(at < width, first, second))
                    mixed = jnp.where(lane >= (at & (width - 1)), behind, ahead)
                    part = weight[b] * lanes_rolled(mixed, (2 * width - start) & (width - 1))
                    total = part if total is None else total + part
                finished[item, m] = total

        small = [
            pltpu.make_async_copy(source, target, small_sem.at[n])
            for n, (source, target) in enumerate(((shift_hbm, shift_ref), (offset_hbm, offset_ref),
                                                  (time_hbm, time_ref), (weight_hbm, weight_ref)))
        ]
        for variable in range(variables):
            for row in (1, 0):
                stage_in(row, variable).start()
            if variable == 0:
                for copy in small:
                    copy.start()

        barrier = pltpu.get_barrier_semaphore()
        for step in range(1, insts):
            pl.semaphore_signal(barrier, inc=1, device_id={"inst": peer(step)}, device_id_type=MESH)
        for step in range(1, strips):
            pl.semaphore_signal(barrier, inc=1, device_id={"pitch": along(step)}, device_id_type=MESH)
        pl.semaphore_wait(barrier, insts + strips - 2)

        @pl.loop(0, items)
        def _(item):
            row, variable, inner = place(item)

            @pl.when(inner == 0)
            def _():
                stage_in(1 - row, variable).wait()
            for step in range(1, insts):
                by_owner(inst, lambda size, step=step: bring(item, step, size).start())

        for copy in small:
            copy.wait()
        plan()

        @pl.loop(0, items + LEAD)
        def _(tick):
            @pl.when(tick < items)
            def _():
                row, variable, inner = place(tick)
                for k in range(inst_dev):
                    raw[tick, inst * inst_dev + k] = stage[1 - row, k, variable, rows_of(inst, inner), :]
                for step in range(1, insts):
                    by_owner(peer(insts - step), lambda size, step=step: bring(tick, step, size).wait_recv())
                resample(tick)
                pack(tick)

            @pl.when(tick == items)
            def _():
                edge_out[...] = gather_edges(items - 1, 1)
                move_edge().start()

            @pl.when(tick >= LEAD)
            def _():
                item = tick - LEAD
                interpolate(item)
                for step in range(1, insts):
                    by_owner(peer(step), lambda size, step=step: give(item, step, size).start())
                by_owner(inst, lambda size: keep(item, size).start())

        @pl.loop(0, items)
        def _(item):
            for step in range(1, insts):
                by_owner(inst, lambda size, step=step: bring(item, step, size).wait_send())
                by_owner(peer(step), lambda size, step=step: give(item, step, size).wait_send())
                by_owner(inst, lambda size, step=step: give(item, step, size).wait_recv())
            by_owner(inst, lambda size: keep(item, size).wait())
            move_near(item).wait_send()
            move_far(item).wait_send()
        move_edge().wait_send()

    vmem, dma = pltpu.VMEM, pltpu.SemaphoreType.DMA
    tile = (TILE, width)
    scratch = [
        pltpu.SMEM((count, 2, count), jnp.float32),
        pltpu.SMEM((count,), jnp.int32),
        pltpu.SMEM((2, members), jnp.int32),
        vmem((2, members, width), jnp.float32),
        dma((4,)),
        vmem((2, inst_dev, variables, span_dev, width), jnp.float32),
        dma((2, variables)),
        vmem((items, slots) + tile, jnp.float32),
        vmem((items, count) + tile, jnp.float32),
        vmem((items, slots) + tile, jnp.float32),
        vmem((items, tiles) + tile, jnp.float32),
        vmem((items, tiles) + tile, jnp.float32),
        vmem(tile, jnp.float32),
        vmem(tile, jnp.float32),
        vmem((tiles,) + tile, jnp.float32),
        vmem(tile, jnp.float32),
        vmem((2, 2, count) + tile, jnp.int32),
        vmem((2, 2) + tile, jnp.int32),
        pltpu.SMEM((14 * count,), jnp.int32),
        dma((items, insts - 1)), dma((items, insts - 1)),
        dma((items,)), dma((items,)), dma((items,)), dma((items,)), dma((1,)), dma((1,)),
        dma((items, insts - 1)), dma((items, insts - 1)), dma((items,)),
    ]
    return kernel, scratch


def make_pick(count, width, budgets):
    def kernel(shift_ref, pick_ref):
        near = jnp.int32(0)
        far = jnp.int32(0)
        edge = jnp.int32(0)
        for m in range(count):
            shift = shift_ref[m]
            for piece in range(2):
                low = shift - REACH - width * (piece + 1)
                size = jnp.clip(low + width + 2 * REACH, 0, width) - jnp.clip(low, 0, width)
                near, far = (near + size, far) if piece == 0 else (near, far + size)
            edge = edge + jnp.where((shift < REACH) | (shift + REACH > 2 * width), EDGE, 0)
        near = (((near + (EDGE - 1)) >> 2) << 2) + edge
        pick = jnp.int32(len(budgets) - 1)
        for n in reversed(range(len(budgets) - 1)):
            fits = (near <= width * budgets[n][0]) & (far <= width * budgets[n][1])
            pick = jnp.where(fits, n, pick)
        pick_ref[0] = pick

    return kernel


def solution(mesh):
    insts, strips = mesh.shape["inst"], mesh.shape["pitch"]

    def on_device(donor_state, time_shift, face_shift, weights, offsets):
        _, inst_dev, variables, span_dev, width = donor_state.shape
        count = time_shift.shape[1]
        members = weights.shape[1]
        hbm = pl.BlockSpec(memory_space=pltpu.HBM)
        sizes = (insts, strips, count, inst_dev, variables, span_dev, width, members)

        def call(made, number):
            kernel, scratch = made
            return pl.pallas_call(
                kernel,
                out_shape=jax.ShapeDtypeStruct(donor_state.shape, jnp.float32),
                in_specs=[hbm] * 5,
                out_specs=pl.BlockSpec(memory_space=pl.ANY),
                scratch_shapes=scratch,
                compiler_params=pltpu.CompilerParams(
                    collective_id=number, has_side_effects=True, vmem_limit_bytes=48 * 1024 * 1024
                ),
            )

        operands = (jnp.transpose(time_shift, (1, 0, 2)), face_shift, offsets, weights, donor_state)
        if strips == 4 and width & (width - 1) == 0 and count * EDGE <= width:
            budgets = BUDGETS + ((count + 1, count),)
            smem = pl.BlockSpec(memory_space=pltpu.SMEM)
            pick = pl.pallas_call(
                make_pick(count, width, budgets),
                out_shape=jax.ShapeDtypeStruct((1,), jnp.int32),
                in_specs=[smem],
                out_specs=smem,
            )(face_shift)[0]
            calls = [call(make_compact(*sizes, *budget), n) for n, budget in enumerate(budgets)]
            received = lax.switch(pick, calls, *operands)
        else:
            received = call(make_general(*sizes), 0)(*operands)
        ids = lax.axis_index("inst") * inst_dev + jnp.arange(inst_dev, dtype=jnp.int32)
        return jnp.where((ids < count)[None, :, None, None, None], received, 0.0)

    return jax.shard_map(
        on_device,
        mesh=mesh,
        in_specs=(P(None, "inst", None, "span", "pitch"), P(), P(), P(None, None, "pitch"), P()),
        out_specs=P(None, "inst", None, "span", "pitch"),
        check_vma=False,
    )
```

```python
import jax
import jax.numpy as jnp
from jax import lax
from jax.experimental import pallas as pl
from jax.experimental.pallas import tpu as pltpu
from jax.sharding import PartitionSpec as P

MESH = pl.DeviceIdType.MESH
TILE = 8
EDGE = 4
REACH = 3
LEAD = 8
BUDGETS = (
    (10, 3), (9, 4), (8, 5), (10, 4), (9, 5), (11, 4), (8, 6), (10, 5), (12, 4), (9, 6),
    (11, 5), (8, 7), (10, 6), (9, 7), (10, 7), (12, 6), (9, 8), (9, 10), (13, 8),
)


def lanes_rolled(value, amount):
    return pltpu.roll(value, amount, 1)


def make_general(insts, strips, count, inst_dev, variables, span_dev, width, band_members):
    band = span_dev // insts
    parts = band // TILE
    chunks = variables * parts
    rounds = max(0, (strips // 2 - 1).bit_length())
    whole_owners, rest = divmod(count, inst_dev)
    slots = insts * inst_dev
    far = sorted({step % strips for bit in range(rounds) for step in (2**bit, -(2**bit))}
                 | {step % strips for step in (1, -1, 2, -2)} - {0})

    def kernel(time_hbm, shift_hbm, offset_hbm, weight_hbm, donor_ref, out_ref,
               time_ref, shift_ref, offset_ref, weight_ref, small_sem, raw, states, edges_out, edges_in, finished,
               in_send, in_recv, local_sem, move_send, move_recv, edge_send, edge_recv,
               out_send, out_recv, keep_sem):
        inst = lax.axis_index("inst")
        strip = lax.axis_index("pitch")

        def peer(step):
            return lax.rem(inst + step, insts)

        def along(step):
            return lax.rem(strip + (step % strips), strips)

        def place(chunk):
            variable = chunk // parts
            return variable, (chunk - variable * parts) * TILE

        def rows_of(owner, inner):
            return pl.ds(pl.multiple_of(owner * band + inner, TILE), TILE)

        def bring(chunk, step, size):
            variable, inner = place(chunk)
            target = peer(step)
            return pltpu.make_async_remote_copy(
                src_ref=donor_ref.at[:, pl.ds(0, size), variable, rows_of(target, inner), :],
                dst_ref=raw.at[chunk, :, pl.ds(inst * inst_dev, size)],
                send_sem=in_send.at[chunk, step - 1],
                recv_sem=in_recv.at[chunk, step - 1],
                device_id={"inst": target},
                device_id_type=MESH,
            )

        def bring_own(chunk):
            variable, inner = place(chunk)
            return pltpu.make_async_copy(
                donor_ref.at[:, :, variable, rows_of(inst, inner), :],
                raw.at[chunk, :, pl.ds(inst * inst_dev, inst_dev)],
                local_sem.at[chunk],
            )

        def move(chunk, row, turn):
            step = 2**turn if turn < rounds else 1
            return pltpu.make_async_remote_copy(
                src_ref=states.at[2 * turn, chunk, row],
                dst_ref=states.at[2 * turn + 1, chunk, row],
                send_sem=move_send.at[chunk, row, turn],
                recv_sem=move_recv.at[chunk, row, turn],
                device_id={"pitch": along(-step if row == 0 else step)},
                device_id_type=MESH,
            )

        def edge_step(row, side):
            if row == 0:
                return -2 if side == 0 else 1
            return -1 if side == 0 else 2

        def move_edge(chunk, row, side):
            return pltpu.make_async_remote_copy(
                src_ref=edges_out.at[chunk, row, side],
                dst_ref=edges_in.at[chunk, row, side],
                send_sem=edge_send.at[chunk, row, side],
                recv_sem=edge_recv.at[chunk, row, side],
                device_id={"pitch": along(edge_step(row, side))},
                device_id_type=MESH,
            )

        def give(chunk, step, size):
            variable, inner = place(chunk)
            target = peer(step)
            return pltpu.make_async_remote_copy(
                src_ref=finished.at[chunk, :, pl.ds(target * inst_dev, size)],
                dst_ref=out_ref.at[:, pl.ds(0, size), variable, rows_of(inst, inner), :],
                send_sem=out_send.at[chunk, step - 1],
                recv_sem=out_recv.at[chunk, step - 1],
                device_id={"inst": target},
                device_id_type=MESH,
            )

        def keep(chunk, size):
            variable, inner = place(chunk)
            return pltpu.make_async_copy(
                finished.at[chunk, :, pl.ds(inst * inst_dev, size)],
                out_ref.at[:, pl.ds(0, size), variable, rows_of(inst, inner), :],
                keep_sem.at[chunk],
            )

        def by_owner(owner, act):
            @pl.when(owner < whole_owners)
            def _():
                act(inst_dev)

            if rest:
                @pl.when(owner == whole_owners)
                def _():
                    act(rest)

        def select_bit(row, index, bit):
            if bit < 0:
                return None
            level = jnp.full((TILE, width), shift_ref[index] // width, jnp.int32)
            return (level & (1 << bit)) != 0

        def resample(chunk):
            for row in range(2):
                donors = [raw[chunk, 1 - row, k] for k in range(count)]

                for m in range(count):
                    total = time_ref[m, row, 0] * donors[0]
                    for k in range(1, count):
                        total = total + time_ref[m, row, k] * donors[k]
                    states[0, chunk, row, m] = total

        def send_turn(chunk, turn):
            for row in range(2):
                move(chunk, row, turn).start()

        def pack_edges(chunk):
            lane = lax.broadcasted_iota(jnp.int32, (TILE, width), 1)
            for row in range(2):
                low = jnp.zeros((TILE, width), jnp.float32)
                high = jnp.zeros((TILE, width), jnp.float32)
                for m in range(count):
                    value = states[2 * rounds, chunk, row, m]
                    here = (lane >= EDGE * m) & (lane < EDGE * (m + 1))
                    low = jnp.where(here, lanes_rolled(value, EDGE * m), low)
                    high = jnp.where(here, lanes_rolled(value, (EDGE * (m + 1)) % width), high)
                edges_out[chunk, row, 0] = low
                edges_out[chunk, row, 1] = high

        def take_turn(chunk, turn):
            for row in range(2):
                move(chunk, row, turn).wait_recv()
                for m in range(count):
                    states[2 * turn + 2, chunk, row, m] = jnp.where(
                        select_bit(row, m, turn),
                        states[2 * turn + 1, chunk, row, m],
                        states[2 * turn, chunk, row, m],
                    )

        def send_fine(chunk):
            send_turn(chunk, rounds)
            pack_edges(chunk)
            for row in range(2):
                for side in range(2):
                    move_edge(chunk, row, side).start()

        def interpolate(chunk):
            lane = lax.broadcasted_iota(jnp.int32, (TILE, width), 1)
            for row in range(2):
                move(chunk, row, rounds).wait_recv()
                for side in range(2):
                    move_edge(chunk, row, side).wait_recv()
                above = edges_in[chunk, row, 0]
                below = edges_in[chunk, row, 1]
                weight = [jnp.broadcast_to(weight_ref[row, b][None, :], (TILE, width)) for b in range(band_members)]
                for m in range(count):
                    own = states[2 * rounds, chunk, row, m]
                    near = states[2 * rounds + 1, chunk, row, m]
                    first, second = (own, near) if row == 0 else (near, own)
                    after = lanes_rolled(above, (width - EDGE * m) % width)
                    before = lanes_rolled(below, (2 * width - EDGE * (m + 1)) % width)
                    inner = lax.rem(shift_ref[m], width)
                    base = inner if row == 0 else width - inner
                    total = None
                    for b in range(band_members):
                        start = base + offset_ref[row, b]
                        at = jnp.full((TILE, width), start, jnp.int32)
                        ahead = jnp.where(at < 0, first, jnp.where(at < width, second, after))
                        behind = jnp.where(at < 0, before, jnp.where(at < width, first, second))
                        turn = at & (width - 1)
                        mixed = jnp.where(lane >= turn, behind, ahead)
                        back = lax.rem(2 * width - start, width)
                        part = weight[b] * lanes_rolled(mixed, back)
                        total = part if total is None else total + part
                    finished[chunk, row, m] = total

        small = [
            pltpu.make_async_copy(source, target, small_sem.at[n])
            for n, (source, target) in enumerate(((shift_hbm, shift_ref), (offset_hbm, offset_ref),
                                                  (time_hbm, time_ref), (weight_hbm, weight_ref)))
        ]
        for copy in small:
            copy.start()

        barrier = pltpu.get_barrier_semaphore()
        for step in range(1, insts):
            pl.semaphore_signal(barrier, inc=1, device_id={"inst": peer(step)}, device_id_type=MESH)
        for step in far:
            pl.semaphore_signal(barrier, inc=1, device_id={"pitch": along(step)}, device_id_type=MESH)
        pl.semaphore_wait(barrier, insts - 1 + len(far))

        @pl.loop(0, chunks)
        def _(chunk):
            bring_own(chunk).start()
            for step in range(1, insts):
                by_owner(inst, lambda size, step=step: bring(chunk, step, size).start())

        for copy in small:
            copy.wait()
        lead = rounds + 1

        @pl.loop(0, chunks + lead)
        def _(tick):
            @pl.when(tick < chunks)
            def _():
                bring_own(tick).wait()
                for step in range(1, insts):
                    by_owner(peer(insts - step), lambda size, step=step: bring(tick, step, size).wait_recv())
                resample(tick)
                if rounds:
                    send_turn(tick, 0)
                else:
                    send_fine(tick)

            for turn in range(rounds):
                @pl.when((tick >= turn + 1) & (tick < chunks + turn + 1))
                def _(turn=turn):
                    chunk = tick - turn - 1
                    take_turn(chunk, turn)
                    if turn + 1 < rounds:
                        send_turn(chunk, turn + 1)
                    else:
                        send_fine(chunk)

            @pl.when(tick >= lead)
            def _():
                chunk = tick - lead
                interpolate(chunk)
                for step in range(1, insts):
                    by_owner(peer(step), lambda size, step=step: give(chunk, step, size).start())
                by_owner(inst, lambda size: keep(chunk, size).start())

        @pl.loop(0, chunks)
        def _(chunk):
            for step in range(1, insts):
                by_owner(inst, lambda size, step=step: bring(chunk, step, size).wait_send())
                by_owner(peer(step), lambda size, step=step: give(chunk, step, size).wait_send())
                by_owner(inst, lambda size, step=step: give(chunk, step, size).wait_recv())
            by_owner(inst, lambda size: keep(chunk, size).wait())
            for row in range(2):
                for turn in range(rounds + 1):
                    move(chunk, row, turn).wait_send()
                for side in range(2):
                    move_edge(chunk, row, side).wait_send()

    vmem, dma = pltpu.VMEM, pltpu.SemaphoreType.DMA
    legs = rounds + 1
    scratch = [
        pltpu.SMEM((count, 2, count), jnp.float32),
        pltpu.SMEM((count,), jnp.int32),
        pltpu.SMEM((2, band_members), jnp.int32),
        vmem((2, band_members, width), jnp.float32),
        dma((4,)),
        vmem((chunks, 2, slots, TILE, width), jnp.float32),
        vmem((2 * rounds + 2, chunks, 2, count, TILE, width), jnp.float32),
        vmem((chunks, 2, 2, TILE, width), jnp.float32),
        vmem((chunks, 2, 2, TILE, width), jnp.float32),
        vmem((chunks, 2, slots, TILE, width), jnp.float32),
        dma((chunks, insts - 1)), dma((chunks, insts - 1)), dma((chunks,)),
        dma((chunks, 2, legs)), dma((chunks, 2, legs)),
        dma((chunks, 2, 2)), dma((chunks, 2, 2)),
        dma((chunks, insts - 1)), dma((chunks, insts - 1)), dma((chunks,)),
    ]
    return kernel, scratch


def make_compact(insts, strips, count, inst_dev, variables, span_dev, width, members, near, far):
    band = span_dev // insts
    parts = band // TILE
    shift_bits = width.bit_length() - 1
    per = 2 * parts
    items = variables * per
    whole_owners, rest = divmod(count, inst_dev)
    slots = insts * inst_dev
    tiles = near + far
    first_tile, piece_tiles = (0, near), (near, far)

    def kernel(time_hbm, shift_hbm, offset_hbm, weight_hbm, donor_ref, out_ref,
               time_ref, shift_ref, offset_ref, weight_ref, small_sem, stage, stage_sem, raw, states, finished,
               packed_out, packed_in, edge_out, edge_in, opened, edge_now, tile_ids, edge_ids, table,
               in_send, in_recv, z_send, z_recv, out_sem):
        inst = lax.axis_index("inst")
        strip = lax.axis_index("pitch")

        def peer(step):
            return lax.rem(inst + step, insts)

        def along(step):
            return lax.rem(strip + strips + step, strips)

        def place(item):
            chunk = item // 2
            variable = chunk // parts
            return item - 2 * chunk, variable, (chunk - variable * parts) * TILE

        def rows_of(owner, inner):
            return pl.ds(pl.multiple_of(owner * band + inner, TILE), TILE)

        def drain(ref, sem):
            pltpu.make_async_copy(ref, ref, sem).wait()

        def stage_in(row, first, size, sem):
            part = pl.ds(first, size)
            return pltpu.make_async_copy(donor_ref.at[row, :, part], stage.at[row, :, part], stage_sem.at[sem])

        def bring(item, step, size):
            row, variable, inner = place(item)
            target = peer(step)
            return pltpu.make_async_remote_copy(
                src_ref=stage.at[1 - row, pl.ds(0, size), variable, rows_of(target, inner), :],
                dst_ref=raw.at[item, pl.ds(inst * inst_dev, size)],
                send_sem=in_send.at[0],
                recv_sem=in_recv.at[jnp.where(item < per, item, per + item // per - 1)],
                device_id={"inst": target},
                device_id_type=MESH,
            )

        def move_near(item):
            row = item - 2 * (item // 2)
            return pltpu.make_async_remote_copy(
                src_ref=packed_out.at[item, pl.ds(0, near)],
                dst_ref=packed_in.at[item, pl.ds(0, near)],
                send_sem=z_send.at[0],
                recv_sem=z_recv.at[item],
                device_id={"pitch": along(2 * row - 1)},
                device_id_type=MESH,
            )

        def move_far(item):
            return pltpu.make_async_remote_copy(
                src_ref=packed_out.at[item, pl.ds(near, far)],
                dst_ref=packed_in.at[item, pl.ds(near, far)],
                send_sem=z_send.at[0],
                recv_sem=z_recv.at[item + 1],
                device_id={"pitch": along(2)},
                device_id_type=MESH,
            )

        def move_edge():
            return pltpu.make_async_remote_copy(
                src_ref=edge_out,
                dst_ref=edge_in,
                send_sem=z_send.at[1],
                recv_sem=z_recv.at[items],
                device_id={"pitch": along(-1)},
                device_id_type=MESH,
            )

        def give(item, step, size):
            row, variable, inner = place(item)
            target = peer(step)
            return pltpu.make_async_remote_copy(
                src_ref=finished.at[item, pl.ds(target * inst_dev, size)],
                dst_ref=out_ref.at[row, pl.ds(0, size), variable, rows_of(inst, inner), :],
                send_sem=out_sem.at[0],
                recv_sem=out_sem.at[1],
                device_id={"inst": target},
                device_id_type=MESH,
            )

        def keep(item, size):
            row, variable, inner = place(item)
            return pltpu.make_async_copy(
                finished.at[item, pl.ds(inst * inst_dev, size)],
                out_ref.at[row, pl.ds(0, size), variable, rows_of(inst, inner), :],
                out_sem.at[2],
            )

        def by_owner(owner, act):
            @pl.when(owner < whole_owners)
            def _():
                act(inst_dev)

            if rest:
                @pl.when(owner == whole_owners)
                def _():
                    act(rest)

        def lanes():
            return lax.broadcasted_iota(jnp.int32, (TILE, width), 1)

        def full(value):
            return jnp.full((TILE, width), value, jnp.int32)

        def edge_amount(row, m):
            ends_high = (shift_ref[m] < width) == (row == 0)
            return table[4 * count * 3 + row * count + m] - jnp.where(ends_high, width - EDGE, 0)

        def plan(row):
            lane = lanes()
            for piece in range(2):
                begin = jnp.int32(0)
                origin = width * (piece + 1)
                for m in range(count):
                    shift = shift_ref[m]
                    low = jnp.where(row == 0, shift, 2 * origin - shift) - REACH - origin
                    start = jnp.clip(low, 0, width)
                    stop = jnp.clip(low + width + 2 * REACH, 0, width)
                    moved = begin - start + width
                    source = (lane - full(moved)) & (width - 1)
                    tile = ((source + full(moved)) >> shift_bits) - 1
                    inside = (source >= full(start)) & (source < full(stop))
                    tile_ids[row, piece, m] = jnp.where(inside, tile, -1)
                    at = ((row * 2 + piece) * count + m) * 3
                    table[at] = moved & (width - 1)
                    tile0 = (moved >> shift_bits) - 1
                    table[at + 1] = jnp.clip(tile0, 0, piece_tiles[piece] - 1) + first_tile[piece]
                    table[at + 2] = jnp.clip(tile0 + 1, 0, piece_tiles[piece] - 1) + first_tile[piece]
                    begin = begin + stop - start
                if piece == 0:
                    begin = ((begin + (EDGE - 1)) >> 2) << 2
                    owner, spot = jnp.full((TILE, width), -1, jnp.int32), jnp.full((TILE, width), -1, jnp.int32)
                    for m in range(count):
                        shift = shift_ref[m]
                        needed = ((shift < REACH) | (shift + REACH > 2 * width)).astype(jnp.int32)
                        at_lane = begin & (width - 1)
                        here = (lane >= full(at_lane)) & (lane < full(at_lane + EDGE * needed))
                        owner = jnp.where(here, m, owner)
                        spot = jnp.where(here, full(begin >> shift_bits), spot)
                        table[4 * count * 3 + (1 - row) * count + m] = at_lane
                        begin = begin + EDGE * needed
                    edge_ids[1 - row, 0] = owner
                    edge_ids[1 - row, 1] = spot

        def resample(item):
            row = item - 2 * (item // 2)
            donors = [raw[item, k] for k in range(count)]
            for m in range(count):
                total = time_ref[m, row, 0] * donors[0]
                for k in range(1, count):
                    total = total + time_ref[m, row, k] * donors[k]
                states[item, m] = total

        def gather_edges(item, row):
            owner = edge_ids[row, 0]
            edge = jnp.zeros((TILE, width), jnp.float32)
            for m in range(count):
                amount = edge_amount(row, m) & (width - 1)
                edge = jnp.where(owner == m, lanes_rolled(states[item, m], amount), edge)
            return edge

        def pack(item):
            row = item - 2 * (item // 2)
            for piece in (1, 0):
                out = [jnp.zeros((TILE, width), jnp.float32)] * piece_tiles[piece]
                for m in range(count):
                    at = ((row * 2 + piece) * count + m) * 3
                    turned = lanes_rolled(states[item, m], table[at])
                    ids = tile_ids[row, piece, m]
                    out = [jnp.where(ids == t, turned, out[t]) for t in range(piece_tiles[piece])]
                if piece == 0:
                    edge = gather_edges(jnp.maximum(item - 1, 0), 1 - row)
                    spot = edge_ids[1 - row, 1]
                    out = [jnp.where(spot == t, edge, out[t]) for t in range(near)]
                for t in range(piece_tiles[piece]):
                    packed_out[item, first_tile[piece] + t] = out[t]
                (move_far if piece else move_near)(item).start()

        def unpack(row, piece, m, lane):
            at = ((row * 2 + piece) * count + m) * 3
            turn = table[at]
            both = jnp.where(lane >= full(turn), opened[table[at + 1]], opened[table[at + 2]])
            return lanes_rolled(both, (width - turn) & (width - 1))

        def interpolate(item):
            row = item - 2 * (item // 2)
            lane = lanes()

            @pl.when(item == 0)
            def _():
                drain(packed_in.at[0, pl.ds(0, near)], z_recv.at[0])

            @pl.when(item + 1 < items)
            def _():
                drain(packed_in.at[item], z_recv.at[item + 1])
                spot = edge_ids[row, 1]
                edge = jnp.zeros((TILE, width), jnp.float32)
                for t in range(near):
                    edge = jnp.where(spot == t, packed_in[item + 1, t], edge)
                edge_now[...] = edge

            @pl.when(item + 1 == items)
            def _():
                drain(packed_in.at[item, pl.ds(0, far + 1)], z_recv.at[items])
                edge_now[...] = edge_in[...]

            for t in range(tiles):
                opened[t] = packed_in[item, t]
            edge = edge_now[...]
            weight = [jnp.broadcast_to(weight_ref[row, b][None, :], (TILE, width)) for b in range(members)]
            forward = full(row) == 0
            for m in range(count):
                strip0 = states[item, m]
                strip1 = unpack(row, 0, m, lane)
                strip2 = unpack(row, 1, m, lane)
                shift = shift_ref[m]
                strip3 = lanes_rolled(edge, (2 * width - edge_amount(row, m)) & (width - 1))
                large = full(shift) >= width
                line = [jnp.where(large, strip0, strip3), jnp.where(large, strip1, strip0),
                        jnp.where(large, strip2, strip1), jnp.where(large, strip3, strip2)]
                before, first = jnp.where(forward, line[0], line[3]), jnp.where(forward, line[1], line[2])
                second, after = jnp.where(forward, line[2], line[1]), jnp.where(forward, line[3], line[0])
                inner = shift & (width - 1)
                base = jnp.where(row == 0, inner, width - inner)
                total = None
                for b in range(members):
                    start = base + offset_ref[row, b]
                    at = full(start)
                    ahead = jnp.where(at < 0, first, jnp.where(at < width, second, after))
                    behind = jnp.where(at < 0, before, jnp.where(at < width, first, second))
                    mixed = jnp.where(lane >= (at & (width - 1)), behind, ahead)
                    part = weight[b] * lanes_rolled(mixed, (2 * width - start) & (width - 1))
                    total = part if total is None else total + part
                finished[item, m] = total

        small = [
            pltpu.make_async_copy(source, target, small_sem.at[n])
            for n, (source, target) in enumerate(((shift_hbm, shift_ref), (offset_hbm, offset_ref),
                                                  (time_hbm, time_ref), (weight_hbm, weight_ref)))
        ]
        stage_in(1, 0, 1, 0).start()
        stage_in(0, 0, 1, 1).start()
        for copy in small:
            copy.start()
        if variables > 1:
            for row in (1, 0):
                stage_in(row, 1, variables - 1, 2).start()

        barrier = pltpu.get_barrier_semaphore()
        for step in range(1, insts):
            pl.semaphore_signal(barrier, inc=1, device_id={"inst": peer(step)}, device_id_type=MESH)
        for step in range(1, strips):
            pl.semaphore_signal(barrier, inc=1, device_id={"pitch": along(step)}, device_id_type=MESH)
        pl.semaphore_wait(barrier, insts + strips - 2)

        @pl.loop(0, items)
        def _(item):
            @pl.when(item == 0)
            def _():
                stage_in(1, 0, 1, 0).wait()

            @pl.when(item == 1)
            def _():
                stage_in(0, 0, 1, 1).wait()

            if variables > 1:
                @pl.when(item == per)
                def _():
                    drain(stage.at[:, :, pl.ds(1, variables - 1)], stage_sem.at[2])
            for step in range(1, insts):
                by_owner(inst, lambda size, step=step: bring(item, step, size).start())

        for copy in small:
            copy.wait()
        pl.loop(0, 2)(plan)

        @pl.loop(0, items + LEAD)
        def _(tick):
            @pl.when(tick < items)
            def _():
                row, variable, inner = place(tick)
                for k in range(inst_dev):
                    raw[tick, inst * inst_dev + k] = stage[1 - row, k, variable, rows_of(inst, inner), :]

                @pl.when(tick < per)
                def _():
                    by_owner(inst, lambda size: drain(raw.at[tick, pl.ds(0, count - size)], in_recv.at[tick]))

                @pl.when((tick >= per) & (inner + row == 0))
                def _():
                    by_owner(inst, lambda size: drain(
                        raw.at[pl.ds(tick, per), pl.ds(0, count - size)], in_recv.at[per + variable - 1]))
                resample(tick)
                pack(tick)

            @pl.when(tick == items)
            def _():
                edge_out[...] = gather_edges(items - 1, 1)
                move_edge().start()

            @pl.when(tick >= LEAD)
            def _():
                item = tick - LEAD
                interpolate(item)
                for step in range(1, insts):
                    by_owner(peer(step), lambda size, step=step: give(item, step, size).start())
                by_owner(inst, lambda size: keep(item, size).start())

        def finish(size):
            drain(raw.at[:, pl.ds(0, (insts - 1) * size)], in_send.at[0])
            drain(finished.at[:, pl.ds(0, count - size)], out_sem.at[0])
            drain(finished.at[:, pl.ds(0, size)], out_sem.at[2])
            drain(finished.at[:, pl.ds(0, (insts - 1) * size)], out_sem.at[1])

        drain(packed_out, z_send.at[0])
        drain(edge_out, z_send.at[1])
        by_owner(inst, finish)

    vmem, dma = pltpu.VMEM, pltpu.SemaphoreType.DMA
    tile = (TILE, width)
    scratch = [
        pltpu.SMEM((count, 2, count), jnp.float32),
        pltpu.SMEM((count,), jnp.int32),
        pltpu.SMEM((2, members), jnp.int32),
        vmem((2, members, width), jnp.float32),
        dma((4,)),
        vmem((2, inst_dev, variables, span_dev, width), jnp.float32),
        dma((3,)),
        vmem((items, slots) + tile, jnp.float32),
        vmem((items, count) + tile, jnp.float32),
        vmem((items, slots) + tile, jnp.float32),
        vmem((items, tiles) + tile, jnp.float32),
        vmem((items, tiles) + tile, jnp.float32),
        vmem(tile, jnp.float32),
        vmem(tile, jnp.float32),
        vmem((tiles,) + tile, jnp.float32),
        vmem(tile, jnp.float32),
        vmem((2, 2, count) + tile, jnp.int32),
        vmem((2, 2) + tile, jnp.int32),
        pltpu.SMEM((14 * count,), jnp.int32),
        dma((1,)), dma((per + variables - 1,)), dma((2,)), dma((items + 1,)), dma((3,)),
    ]
    return kernel, scratch


def make_pick(count, width, budgets):
    def kernel(shift_ref, pick_ref):
        near = jnp.int32(0)
        far = jnp.int32(0)
        edge = jnp.int32(0)
        for m in range(count):
            shift = shift_ref[m]
            for piece in range(2):
                low = shift - REACH - width * (piece + 1)
                size = jnp.clip(low + width + 2 * REACH, 0, width) - jnp.clip(low, 0, width)
                near, far = (near + size, far) if piece == 0 else (near, far + size)
            edge = edge + jnp.where((shift < REACH) | (shift + REACH > 2 * width), EDGE, 0)
        near = (((near + (EDGE - 1)) >> 2) << 2) + edge
        pick = jnp.int32(len(budgets) - 1)
        for n in reversed(range(len(budgets) - 1)):
            fits = (near <= width * budgets[n][0]) & (far <= width * budgets[n][1])
            pick = jnp.where(fits, n, pick)
        pick_ref[0] = pick

    return kernel


def solution(mesh):
    insts, strips = mesh.shape["inst"], mesh.shape["pitch"]

    def on_device(donor_state, time_shift, face_shift, weights, offsets):
        _, inst_dev, variables, span_dev, width = donor_state.shape
        count = time_shift.shape[1]
        members = weights.shape[1]
        hbm = pl.BlockSpec(memory_space=pltpu.HBM)
        sizes = (insts, strips, count, inst_dev, variables, span_dev, width, members)

        def call(made, number):
            kernel, scratch = made
            return pl.pallas_call(
                kernel,
                out_shape=jax.ShapeDtypeStruct(donor_state.shape, jnp.float32),
                in_specs=[hbm] * 5,
                out_specs=pl.BlockSpec(memory_space=pl.ANY),
                scratch_shapes=scratch,
                compiler_params=pltpu.CompilerParams(
                    collective_id=number, has_side_effects=True, vmem_limit_bytes=48 * 1024 * 1024
                ),
            )

        operands = (jnp.transpose(time_shift, (1, 0, 2)), face_shift, offsets, weights, donor_state)
        if strips == 4 and width & (width - 1) == 0 and count * EDGE <= width and -(-count // inst_dev) == insts:
            budgets = BUDGETS + ((count + 1, count),)
            smem = pl.BlockSpec(memory_space=pltpu.SMEM)
            pick = pl.pallas_call(
                make_pick(count, width, budgets),
                out_shape=jax.ShapeDtypeStruct((1,), jnp.int32),
                in_specs=[smem],
                out_specs=smem,
            )(face_shift)[0]
            calls = [call(make_compact(*sizes, *budget), n) for n, budget in enumerate(budgets)]
            received = lax.switch(pick, calls, *operands)
        else:
            received = call(make_general(*sizes), 0)(*operands)
        ids = lax.axis_index("inst") * inst_dev + jnp.arange(inst_dev, dtype=jnp.int32)
        return jnp.where((ids < count)[None, :, None, None, None], received, 0.0)

    return jax.shard_map(
        on_device,
        mesh=mesh,
        in_specs=(P(None, "inst", None, "span", "pitch"), P(), P(), P(None, None, "pitch"), P()),
        out_specs=P(None, "inst", None, "span", "pitch"),
        check_vma=False,
    )
```

```python
import jax
import jax.numpy as jnp
from jax import lax
from jax.experimental import pallas as pl
from jax.experimental.pallas import tpu as pltpu
from jax.sharding import PartitionSpec as P

MESH = pl.DeviceIdType.MESH
TILE = 8
EDGE = 4
REACH = 3
LEAD = 8
BUDGETS = (
    (10, 3), (9, 4), (8, 5), (10, 4), (9, 5), (11, 4), (8, 6), (10, 5), (12, 4), (9, 6),
    (11, 5), (8, 7), (10, 6), (9, 7), (10, 7), (12, 6), (9, 8), (9, 10), (13, 8),
)


def lanes_rolled(value, amount):
    return pltpu.roll(value, amount, 1)


def make_general(insts, strips, count, inst_dev, variables, span_dev, width, band_members):
    band = span_dev // insts
    parts = band // TILE
    chunks = variables * parts
    rounds = max(0, (strips // 2 - 1).bit_length())
    whole_owners, rest = divmod(count, inst_dev)
    slots = insts * inst_dev
    far = sorted({step % strips for bit in range(rounds) for step in (2**bit, -(2**bit))}
                 | {step % strips for step in (1, -1, 2, -2)} - {0})

    def kernel(time_hbm, shift_hbm, offset_hbm, weight_hbm, donor_ref, out_ref,
               time_ref, shift_ref, offset_ref, weight_ref, small_sem, raw, states, edges_out, edges_in, finished,
               in_send, in_recv, local_sem, move_send, move_recv, edge_send, edge_recv,
               out_send, out_recv, keep_sem):
        inst = lax.axis_index("inst")
        strip = lax.axis_index("pitch")

        def peer(step):
            return lax.rem(inst + step, insts)

        def along(step):
            return lax.rem(strip + (step % strips), strips)

        def place(chunk):
            variable = chunk // parts
            return variable, (chunk - variable * parts) * TILE

        def rows_of(owner, inner):
            return pl.ds(pl.multiple_of(owner * band + inner, TILE), TILE)

        def bring(chunk, step, size):
            variable, inner = place(chunk)
            target = peer(step)
            return pltpu.make_async_remote_copy(
                src_ref=donor_ref.at[:, pl.ds(0, size), variable, rows_of(target, inner), :],
                dst_ref=raw.at[chunk, :, pl.ds(inst * inst_dev, size)],
                send_sem=in_send.at[chunk, step - 1],
                recv_sem=in_recv.at[chunk, step - 1],
                device_id={"inst": target},
                device_id_type=MESH,
            )

        def bring_own(chunk):
            variable, inner = place(chunk)
            return pltpu.make_async_copy(
                donor_ref.at[:, :, variable, rows_of(inst, inner), :],
                raw.at[chunk, :, pl.ds(inst * inst_dev, inst_dev)],
                local_sem.at[chunk],
            )

        def move(chunk, row, turn):
            step = 2**turn if turn < rounds else 1
            return pltpu.make_async_remote_copy(
                src_ref=states.at[2 * turn, chunk, row],
                dst_ref=states.at[2 * turn + 1, chunk, row],
                send_sem=move_send.at[chunk, row, turn],
                recv_sem=move_recv.at[chunk, row, turn],
                device_id={"pitch": along(-step if row == 0 else step)},
                device_id_type=MESH,
            )

        def edge_step(row, side):
            if row == 0:
                return -2 if side == 0 else 1
            return -1 if side == 0 else 2

        def move_edge(chunk, row, side):
            return pltpu.make_async_remote_copy(
                src_ref=edges_out.at[chunk, row, side],
                dst_ref=edges_in.at[chunk, row, side],
                send_sem=edge_send.at[chunk, row, side],
                recv_sem=edge_recv.at[chunk, row, side],
                device_id={"pitch": along(edge_step(row, side))},
                device_id_type=MESH,
            )

        def give(chunk, step, size):
            variable, inner = place(chunk)
            target = peer(step)
            return pltpu.make_async_remote_copy(
                src_ref=finished.at[chunk, :, pl.ds(target * inst_dev, size)],
                dst_ref=out_ref.at[:, pl.ds(0, size), variable, rows_of(inst, inner), :],
                send_sem=out_send.at[chunk, step - 1],
                recv_sem=out_recv.at[chunk, step - 1],
                device_id={"inst": target},
                device_id_type=MESH,
            )

        def keep(chunk, size):
            variable, inner = place(chunk)
            return pltpu.make_async_copy(
                finished.at[chunk, :, pl.ds(inst * inst_dev, size)],
                out_ref.at[:, pl.ds(0, size), variable, rows_of(inst, inner), :],
                keep_sem.at[chunk],
            )

        def by_owner(owner, act):
            @pl.when(owner < whole_owners)
            def _():
                act(inst_dev)

            if rest:
                @pl.when(owner == whole_owners)
                def _():
                    act(rest)

        def select_bit(row, index, bit):
            if bit < 0:
                return None
            level = jnp.full((TILE, width), shift_ref[index] // width, jnp.int32)
            return (level & (1 << bit)) != 0

        def resample(chunk):
            for row in range(2):
                donors = [raw[chunk, 1 - row, k] for k in range(count)]

                for m in range(count):
                    total = time_ref[m, row, 0] * donors[0]
                    for k in range(1, count):
                        total = total + time_ref[m, row, k] * donors[k]
                    states[0, chunk, row, m] = total

        def send_turn(chunk, turn):
            for row in range(2):
                move(chunk, row, turn).start()

        def pack_edges(chunk):
            lane = lax.broadcasted_iota(jnp.int32, (TILE, width), 1)
            for row in range(2):
                low = jnp.zeros((TILE, width), jnp.float32)
                high = jnp.zeros((TILE, width), jnp.float32)
                for m in range(count):
                    value = states[2 * rounds, chunk, row, m]
                    here = (lane >= EDGE * m) & (lane < EDGE * (m + 1))
                    low = jnp.where(here, lanes_rolled(value, EDGE * m), low)
                    high = jnp.where(here, lanes_rolled(value, (EDGE * (m + 1)) % width), high)
                edges_out[chunk, row, 0] = low
                edges_out[chunk, row, 1] = high

        def take_turn(chunk, turn):
            for row in range(2):
                move(chunk, row, turn).wait_recv()
                for m in range(count):
                    states[2 * turn + 2, chunk, row, m] = jnp.where(
                        select_bit(row, m, turn),
                        states[2 * turn + 1, chunk, row, m],
                        states[2 * turn, chunk, row, m],
                    )

        def send_fine(chunk):
            send_turn(chunk, rounds)
            pack_edges(chunk)
            for row in range(2):
                for side in range(2):
                    move_edge(chunk, row, side).start()

        def interpolate(chunk):
            lane = lax.broadcasted_iota(jnp.int32, (TILE, width), 1)
            for row in range(2):
                move(chunk, row, rounds).wait_recv()
                for side in range(2):
                    move_edge(chunk, row, side).wait_recv()
                above = edges_in[chunk, row, 0]
                below = edges_in[chunk, row, 1]
                weight = [jnp.broadcast_to(weight_ref[row, b][None, :], (TILE, width)) for b in range(band_members)]
                for m in range(count):
                    own = states[2 * rounds, chunk, row, m]
                    near = states[2 * rounds + 1, chunk, row, m]
                    first, second = (own, near) if row == 0 else (near, own)
                    after = lanes_rolled(above, (width - EDGE * m) % width)
                    before = lanes_rolled(below, (2 * width - EDGE * (m + 1)) % width)
                    inner = lax.rem(shift_ref[m], width)
                    base = inner if row == 0 else width - inner
                    total = None
                    for b in range(band_members):
                        start = base + offset_ref[row, b]
                        at = jnp.full((TILE, width), start, jnp.int32)
                        ahead = jnp.where(at < 0, first, jnp.where(at < width, second, after))
                        behind = jnp.where(at < 0, before, jnp.where(at < width, first, second))
                        turn = at & (width - 1)
                        mixed = jnp.where(lane >= turn, behind, ahead)
                        back = lax.rem(2 * width - start, width)
                        part = weight[b] * lanes_rolled(mixed, back)
                        total = part if total is None else total + part
                    finished[chunk, row, m] = total

        small = [
            pltpu.make_async_copy(source, target, small_sem.at[n])
            for n, (source, target) in enumerate(((shift_hbm, shift_ref), (offset_hbm, offset_ref),
                                                  (time_hbm, time_ref), (weight_hbm, weight_ref)))
        ]
        for copy in small:
            copy.start()

        barrier = pltpu.get_barrier_semaphore()
        for step in range(1, insts):
            pl.semaphore_signal(barrier, inc=1, device_id={"inst": peer(step)}, device_id_type=MESH)
        for step in far:
            pl.semaphore_signal(barrier, inc=1, device_id={"pitch": along(step)}, device_id_type=MESH)
        pl.semaphore_wait(barrier, insts - 1 + len(far))

        @pl.loop(0, chunks)
        def _(chunk):
            bring_own(chunk).start()
            for step in range(1, insts):
                by_owner(inst, lambda size, step=step: bring(chunk, step, size).start())

        for copy in small:
            copy.wait()
        lead = rounds + 1

        @pl.loop(0, chunks + lead)
        def _(tick):
            @pl.when(tick < chunks)
            def _():
                bring_own(tick).wait()
                for step in range(1, insts):
                    by_owner(peer(insts - step), lambda size, step=step: bring(tick, step, size).wait_recv())
                resample(tick)
                if rounds:
                    send_turn(tick, 0)
                else:
                    send_fine(tick)

            for turn in range(rounds):
                @pl.when((tick >= turn + 1) & (tick < chunks + turn + 1))
                def _(turn=turn):
                    chunk = tick - turn - 1
                    take_turn(chunk, turn)
                    if turn + 1 < rounds:
                        send_turn(chunk, turn + 1)
                    else:
                        send_fine(chunk)

            @pl.when(tick >= lead)
            def _():
                chunk = tick - lead
                interpolate(chunk)
                for step in range(1, insts):
                    by_owner(peer(step), lambda size, step=step: give(chunk, step, size).start())
                by_owner(inst, lambda size: keep(chunk, size).start())

        @pl.loop(0, chunks)
        def _(chunk):
            for step in range(1, insts):
                by_owner(inst, lambda size, step=step: bring(chunk, step, size).wait_send())
                by_owner(peer(step), lambda size, step=step: give(chunk, step, size).wait_send())
                by_owner(inst, lambda size, step=step: give(chunk, step, size).wait_recv())
            by_owner(inst, lambda size: keep(chunk, size).wait())
            for row in range(2):
                for turn in range(rounds + 1):
                    move(chunk, row, turn).wait_send()
                for side in range(2):
                    move_edge(chunk, row, side).wait_send()

    vmem, dma = pltpu.VMEM, pltpu.SemaphoreType.DMA
    legs = rounds + 1
    scratch = [
        pltpu.SMEM((count, 2, count), jnp.float32),
        pltpu.SMEM((count,), jnp.int32),
        pltpu.SMEM((2, band_members), jnp.int32),
        vmem((2, band_members, width), jnp.float32),
        dma((4,)),
        vmem((chunks, 2, slots, TILE, width), jnp.float32),
        vmem((2 * rounds + 2, chunks, 2, count, TILE, width), jnp.float32),
        vmem((chunks, 2, 2, TILE, width), jnp.float32),
        vmem((chunks, 2, 2, TILE, width), jnp.float32),
        vmem((chunks, 2, slots, TILE, width), jnp.float32),
        dma((chunks, insts - 1)), dma((chunks, insts - 1)), dma((chunks,)),
        dma((chunks, 2, legs)), dma((chunks, 2, legs)),
        dma((chunks, 2, 2)), dma((chunks, 2, 2)),
        dma((chunks, insts - 1)), dma((chunks, insts - 1)), dma((chunks,)),
    ]
    return kernel, scratch


def make_compact(insts, strips, count, inst_dev, variables, span_dev, width, members, near, far):
    band = span_dev // insts
    parts = band // TILE
    shift_bits = width.bit_length() - 1
    per = 2 * parts
    items = variables * per
    whole_owners, rest = divmod(count, inst_dev)
    slots = insts * inst_dev
    tiles = near + far
    first_tile, piece_tiles = (0, near), (near, far)

    def kernel(time_hbm, shift_hbm, offset_hbm, weight_hbm, donor_ref, out_ref,
               time_ref, shift_ref, offset_ref, weight_ref, small_sem, stage, stage_sem, raw, states, finished,
               packed_out, packed_in, edge_out, edge_in, opened, edge_now, tile_ids, edge_ids, table,
               in_send, in_recv, z_send, z_recv, out_sem, zeros):
        inst = lax.axis_index("inst")
        strip = lax.axis_index("pitch")

        def peer(step):
            return lax.rem(inst + step, insts)

        def along(step):
            return lax.rem(strip + strips + step, strips)

        def place(item):
            chunk = item // 2
            variable = chunk // parts
            return item - 2 * chunk, variable, (chunk - variable * parts) * TILE

        def rows_of(owner, inner):
            return pl.ds(pl.multiple_of(owner * band + inner, TILE), TILE)

        def drain(ref, sem):
            pltpu.make_async_copy(ref, ref, sem).wait()

        def stage_in(row, first, size, sem):
            part = pl.ds(first, size)
            return pltpu.make_async_copy(donor_ref.at[row, :, part], stage.at[row, :, part], stage_sem.at[sem])

        def bring(item, step, size):
            row, variable, inner = place(item)
            target = peer(step)
            return pltpu.make_async_remote_copy(
                src_ref=stage.at[1 - row, pl.ds(0, size), variable, rows_of(target, inner), :],
                dst_ref=raw.at[item, pl.ds(inst * inst_dev, size)],
                send_sem=in_send.at[0],
                recv_sem=in_recv.at[jnp.where(item < per, item, per + item // per - 1)],
                device_id={"inst": target},
                device_id_type=MESH,
            )

        def move_near(item):
            row = item - 2 * (item // 2)
            return pltpu.make_async_remote_copy(
                src_ref=packed_out.at[item, pl.ds(0, near)],
                dst_ref=packed_in.at[item, pl.ds(0, near)],
                send_sem=z_send.at[0],
                recv_sem=z_recv.at[item],
                device_id={"pitch": along(2 * row - 1)},
                device_id_type=MESH,
            )

        def move_far(item):
            return pltpu.make_async_remote_copy(
                src_ref=packed_out.at[item, pl.ds(near, far)],
                dst_ref=packed_in.at[item, pl.ds(near, far)],
                send_sem=z_send.at[0],
                recv_sem=z_recv.at[item + 1],
                device_id={"pitch": along(2)},
                device_id_type=MESH,
            )

        def move_edge():
            return pltpu.make_async_remote_copy(
                src_ref=edge_out,
                dst_ref=edge_in,
                send_sem=z_send.at[1],
                recv_sem=z_recv.at[items],
                device_id={"pitch": along(-1)},
                device_id_type=MESH,
            )

        def give(item, step, size):
            row, variable, inner = place(item)
            target = peer(step)
            return pltpu.make_async_remote_copy(
                src_ref=finished.at[item, pl.ds(target * inst_dev, size)],
                dst_ref=out_ref.at[row, pl.ds(0, size), variable, rows_of(inst, inner), :],
                send_sem=out_sem.at[0],
                recv_sem=out_sem.at[1],
                device_id={"inst": target},
                device_id_type=MESH,
            )

        def keep(item, size):
            row, variable, inner = place(item)
            return pltpu.make_async_copy(
                finished.at[item, pl.ds(inst * inst_dev, size)],
                out_ref.at[row, pl.ds(0, size), variable, rows_of(inst, inner), :],
                out_sem.at[2],
            )

        def by_owner(owner, act):
            @pl.when(owner < whole_owners)
            def _():
                act(inst_dev)

            if rest:
                @pl.when(owner == whole_owners)
                def _():
                    act(rest)

        def lanes():
            return lax.broadcasted_iota(jnp.int32, (TILE, width), 1)

        def full(value):
            return jnp.full((TILE, width), value, jnp.int32)

        def edge_amount(row, m):
            ends_high = (shift_ref[m] < width) == (row == 0)
            return table[4 * count * 3 + row * count + m] - jnp.where(ends_high, width - EDGE, 0)

        def plan(row):
            lane = lanes()
            for piece in range(2):
                begin = jnp.int32(0)
                origin = width * (piece + 1)
                for m in range(count):
                    shift = shift_ref[m]
                    low = jnp.where(row == 0, shift, 2 * origin - shift) - REACH - origin
                    start = jnp.clip(low, 0, width)
                    stop = jnp.clip(low + width + 2 * REACH, 0, width)
                    moved = begin - start + width
                    source = (lane - full(moved)) & (width - 1)
                    tile = ((source + full(moved)) >> shift_bits) - 1
                    inside = (source >= full(start)) & (source < full(stop))
                    tile_ids[row, piece, m] = jnp.where(inside, tile, -1)
                    at = ((row * 2 + piece) * count + m) * 3
                    table[at] = moved & (width - 1)
                    tile0 = (moved >> shift_bits) - 1
                    table[at + 1] = jnp.clip(tile0, 0, piece_tiles[piece] - 1) + first_tile[piece]
                    table[at + 2] = jnp.clip(tile0 + 1, 0, piece_tiles[piece] - 1) + first_tile[piece]
                    begin = begin + stop - start
                if piece == 0:
                    begin = ((begin + (EDGE - 1)) >> 2) << 2
                    owner, spot = jnp.full((TILE, width), -1, jnp.int32), jnp.full((TILE, width), -1, jnp.int32)
                    for m in range(count):
                        shift = shift_ref[m]
                        needed = ((shift < REACH) | (shift + REACH > 2 * width)).astype(jnp.int32)
                        at_lane = begin & (width - 1)
                        here = (lane >= full(at_lane)) & (lane < full(at_lane + EDGE * needed))
                        owner = jnp.where(here, m, owner)
                        spot = jnp.where(here, full(begin >> shift_bits), spot)
                        table[4 * count * 3 + (1 - row) * count + m] = at_lane
                        begin = begin + EDGE * needed
                    edge_ids[1 - row, 0] = owner
                    edge_ids[1 - row, 1] = spot

        def resample(item):
            row = item - 2 * (item // 2)
            donors = [raw[item, k] for k in range(count)]
            for m in range(count):
                total = time_ref[m, row, 0] * donors[0]
                for k in range(1, count):
                    total = total + time_ref[m, row, k] * donors[k]
                states[item, m] = total

        def gather_edges(item, row):
            owner = edge_ids[row, 0]
            edge = jnp.zeros((TILE, width), jnp.float32)
            for m in range(count):
                amount = edge_amount(row, m) & (width - 1)
                edge = jnp.where(owner == m, lanes_rolled(states[item, m], amount), edge)
            return edge

        def pack(item):
            row = item - 2 * (item // 2)
            for piece in (1, 0):
                out = [jnp.zeros((TILE, width), jnp.float32)] * piece_tiles[piece]
                for m in range(count):
                    at = ((row * 2 + piece) * count + m) * 3
                    turned = lanes_rolled(states[item, m], table[at])
                    ids = tile_ids[row, piece, m]
                    out = [jnp.where(ids == t, turned, out[t]) for t in range(piece_tiles[piece])]
                if piece == 0:
                    edge = gather_edges(jnp.maximum(item - 1, 0), 1 - row)
                    spot = edge_ids[1 - row, 1]
                    out = [jnp.where(spot == t, edge, out[t]) for t in range(near)]
                for t in range(piece_tiles[piece]):
                    packed_out[item, first_tile[piece] + t] = out[t]
                (move_far if piece else move_near)(item).start()

        def unpack(row, piece, m, lane):
            at = ((row * 2 + piece) * count + m) * 3
            turn = table[at]
            both = jnp.where(lane >= full(turn), opened[table[at + 1]], opened[table[at + 2]])
            return lanes_rolled(both, (width - turn) & (width - 1))

        def interpolate(item):
            row = item - 2 * (item // 2)
            lane = lanes()

            @pl.when(item == 0)
            def _():
                drain(packed_in.at[0, pl.ds(0, near)], z_recv.at[0])

            @pl.when(item + 1 < items)
            def _():
                drain(packed_in.at[item], z_recv.at[item + 1])
                spot = edge_ids[row, 1]
                edge = jnp.zeros((TILE, width), jnp.float32)
                for t in range(near):
                    edge = jnp.where(spot == t, packed_in[item + 1, t], edge)
                edge_now[...] = edge

            @pl.when(item + 1 == items)
            def _():
                drain(packed_in.at[item, pl.ds(0, far + 1)], z_recv.at[items])
                edge_now[...] = edge_in[...]

            for t in range(tiles):
                opened[t] = packed_in[item, t]
            edge = edge_now[...]
            weight = [jnp.broadcast_to(weight_ref[row, b][None, :], (TILE, width)) for b in range(members)]
            forward = full(row) == 0
            for m in range(count):
                strip0 = states[item, m]
                strip1 = unpack(row, 0, m, lane)
                strip2 = unpack(row, 1, m, lane)
                shift = shift_ref[m]
                strip3 = lanes_rolled(edge, (2 * width - edge_amount(row, m)) & (width - 1))
                large = full(shift) >= width
                line = [jnp.where(large, strip0, strip3), jnp.where(large, strip1, strip0),
                        jnp.where(large, strip2, strip1), jnp.where(large, strip3, strip2)]
                before, first = jnp.where(forward, line[0], line[3]), jnp.where(forward, line[1], line[2])
                second, after = jnp.where(forward, line[2], line[1]), jnp.where(forward, line[3], line[0])
                inner = shift & (width - 1)
                base = jnp.where(row == 0, inner, width - inner)
                total = None
                for b in range(members):
                    start = base + offset_ref[row, b]
                    at = full(start)
                    ahead = jnp.where(at < 0, first, jnp.where(at < width, second, after))
                    behind = jnp.where(at < 0, before, jnp.where(at < width, first, second))
                    mixed = jnp.where(lane >= (at & (width - 1)), behind, ahead)
                    part = weight[b] * lanes_rolled(mixed, (2 * width - start) & (width - 1))
                    total = part if total is None else total + part
                finished[item, m] = total

        small = [
            pltpu.make_async_copy(source, target, small_sem.at[n])
            for n, (source, target) in enumerate(((shift_hbm, shift_ref), (offset_hbm, offset_ref),
                                                  (time_hbm, time_ref), (weight_hbm, weight_ref)))
        ]
        stage_in(1, 0, 1, 0).start()
        stage_in(0, 0, 1, 1).start()
        for copy in small:
            copy.start()
        if variables > 1:
            for row in (1, 0):
                stage_in(row, 1, variables - 1, 2).start()

        barrier = pltpu.get_barrier_semaphore()
        for step in range(1, insts):
            pl.semaphore_signal(barrier, inc=1, device_id={"inst": peer(step)}, device_id_type=MESH)
        for step in range(1, strips):
            pl.semaphore_signal(barrier, inc=1, device_id={"pitch": along(step)}, device_id_type=MESH)
        pl.semaphore_wait(barrier, insts + strips - 2)

        @pl.loop(0, items)
        def _(item):
            @pl.when(item == 0)
            def _():
                stage_in(1, 0, 1, 0).wait()

            @pl.when(item == 1)
            def _():
                stage_in(0, 0, 1, 1).wait()

            if variables > 1:
                @pl.when(item == per)
                def _():
                    drain(stage.at[:, :, pl.ds(1, variables - 1)], stage_sem.at[2])
            for step in range(1, insts):
                by_owner(inst, lambda size, step=step: bring(item, step, size).start())

        if rest:
            @pl.when(inst == whole_owners)
            def _():
                zeros[...] = jnp.zeros_like(zeros)

        for copy in small:
            copy.wait()
        pl.loop(0, 2)(plan)

        if rest:
            @pl.when(inst == whole_owners)
            def _():
                for row in range(2):
                    for slot in range(rest, inst_dev):
                        pltpu.make_async_copy(zeros, out_ref.at[row, slot], out_sem.at[3]).start()

        @pl.loop(0, items + LEAD)
        def _(tick):
            @pl.when(tick < items)
            def _():
                row, variable, inner = place(tick)
                for k in range(inst_dev):
                    raw[tick, inst * inst_dev + k] = stage[1 - row, k, variable, rows_of(inst, inner), :]

                @pl.when(tick < per)
                def _():
                    by_owner(inst, lambda size: drain(raw.at[tick, pl.ds(0, count - size)], in_recv.at[tick]))

                @pl.when((tick >= per) & (inner + row == 0))
                def _():
                    by_owner(inst, lambda size: drain(
                        raw.at[pl.ds(tick, per), pl.ds(0, count - size)], in_recv.at[per + variable - 1]))
                resample(tick)
                pack(tick)

            @pl.when(tick == items)
            def _():
                edge_out[...] = gather_edges(items - 1, 1)
                move_edge().start()

            @pl.when(tick >= LEAD)
            def _():
                item = tick - LEAD
                interpolate(item)
                for step in range(1, insts):
                    by_owner(peer(step), lambda size, step=step: give(item, step, size).start())
                by_owner(inst, lambda size: keep(item, size).start())

        def finish(size):
            drain(raw.at[:, pl.ds(0, (insts - 1) * size)], in_send.at[0])
            drain(finished.at[:, pl.ds(0, count - size)], out_sem.at[0])
            drain(finished.at[:, pl.ds(0, size)], out_sem.at[2])
            drain(finished.at[:, pl.ds(0, (insts - 1) * size)], out_sem.at[1])
            if size < inst_dev:
                drain(out_ref.at[:, pl.ds(size, inst_dev - size)], out_sem.at[3])

        drain(packed_out, z_send.at[0])
        drain(edge_out, z_send.at[1])
        by_owner(inst, finish)

    vmem, dma = pltpu.VMEM, pltpu.SemaphoreType.DMA
    tile = (TILE, width)
    scratch = [
        pltpu.SMEM((count, 2, count), jnp.float32),
        pltpu.SMEM((count,), jnp.int32),
        pltpu.SMEM((2, members), jnp.int32),
        vmem((2, members, width), jnp.float32),
        dma((4,)),
        vmem((2, inst_dev, variables, span_dev, width), jnp.float32),
        dma((3,)),
        vmem((items, slots) + tile, jnp.float32),
        vmem((items, count) + tile, jnp.float32),
        vmem((items, slots) + tile, jnp.float32),
        vmem((items, tiles) + tile, jnp.float32),
        vmem((items, tiles) + tile, jnp.float32),
        vmem(tile, jnp.float32),
        vmem(tile, jnp.float32),
        vmem((tiles,) + tile, jnp.float32),
        vmem(tile, jnp.float32),
        vmem((2, 2, count) + tile, jnp.int32),
        vmem((2, 2) + tile, jnp.int32),
        pltpu.SMEM((14 * count,), jnp.int32),
        dma((1,)), dma((per + variables - 1,)), dma((2,)), dma((items + 1,)), dma((4,)),
        vmem((variables, span_dev, width), jnp.float32),
    ]
    return kernel, scratch


def make_pick(count, width, budgets):
    def kernel(shift_ref, pick_ref):
        near = jnp.int32(0)
        far = jnp.int32(0)
        edge = jnp.int32(0)
        for m in range(count):
            shift = shift_ref[m]
            for piece in range(2):
                low = shift - REACH - width * (piece + 1)
                size = jnp.clip(low + width + 2 * REACH, 0, width) - jnp.clip(low, 0, width)
                near, far = (near + size, far) if piece == 0 else (near, far + size)
            edge = edge + jnp.where((shift < REACH) | (shift + REACH > 2 * width), EDGE, 0)
        near = (((near + (EDGE - 1)) >> 2) << 2) + edge
        pick = jnp.int32(len(budgets) - 1)
        for n in reversed(range(len(budgets) - 1)):
            fits = (near <= width * budgets[n][0]) & (far <= width * budgets[n][1])
            pick = jnp.where(fits, n, pick)
        pick_ref[0] = pick

    return kernel


def solution(mesh):
    insts, strips = mesh.shape["inst"], mesh.shape["pitch"]

    def on_device(donor_state, time_shift, face_shift, weights, offsets):
        _, inst_dev, variables, span_dev, width = donor_state.shape
        count = time_shift.shape[1]
        members = weights.shape[1]
        hbm = pl.BlockSpec(memory_space=pltpu.HBM)
        sizes = (insts, strips, count, inst_dev, variables, span_dev, width, members)

        def call(made, number):
            kernel, scratch = made
            return pl.pallas_call(
                kernel,
                out_shape=jax.ShapeDtypeStruct(donor_state.shape, jnp.float32),
                in_specs=[hbm] * 5,
                out_specs=pl.BlockSpec(memory_space=pl.ANY),
                scratch_shapes=scratch,
                compiler_params=pltpu.CompilerParams(
                    collective_id=number, has_side_effects=True, vmem_limit_bytes=48 * 1024 * 1024
                ),
            )

        operands = (jnp.transpose(time_shift, (1, 0, 2)), face_shift, offsets, weights, donor_state)
        if strips == 4 and width & (width - 1) == 0 and count * EDGE <= width and -(-count // inst_dev) == insts:
            budgets = BUDGETS + ((count + 1, count),)
            smem = pl.BlockSpec(memory_space=pltpu.SMEM)
            pick = pl.pallas_call(
                make_pick(count, width, budgets),
                out_shape=jax.ShapeDtypeStruct((1,), jnp.int32),
                in_specs=[smem],
                out_specs=smem,
            )(face_shift)[0]
            calls = [call(make_compact(*sizes, *budget), n) for n, budget in enumerate(budgets)]
            return lax.switch(pick, calls, *operands)
        received = call(make_general(*sizes), 0)(*operands)
        ids = lax.axis_index("inst") * inst_dev + jnp.arange(inst_dev, dtype=jnp.int32)
        return jnp.where((ids < count)[None, :, None, None, None], received, 0.0)

    return jax.shard_map(
        on_device,
        mesh=mesh,
        in_specs=(P(None, "inst", None, "span", "pitch"), P(), P(), P(None, None, "pitch"), P()),
        out_specs=P(None, "inst", None, "span", "pitch"),
        check_vma=False,
    )
```
